32 devices in a mesh: pod: 2 (over x), data: 4 (over z), tensor: 4 (over y, core).
Axes of the slice: x: 2, y: 2, z: 4, core: 2. Of those that a mesh axis runs over, the one named last changes fastest.
Arguments:
- token_ids: int32 [32768], P(('pod', 'data')), parts along dimension 0
- embed_table: bfloat16 [50304, 1024], P('tensor')
- norm_gain: bfloat16 [1024], replicated
- w_in: bfloat16 [1024, 4096], P(None, 'tensor')
- w_out: bfloat16 [4096, 1024], P('tensor')
- d_out: bfloat16 [32768, 1024], P(('pod', 'data', 'tensor')), parts along dimension 0
Outputs:
- output 1: bfloat16 [32768, 1024], P(('pod', 'data', 'tensor')), parts along dimension 0
- output 2: float32 [100608, 1024], P(('pod', 'tensor')), parts along dimension 0
- output 3: float32 [2048, 4096], P('pod', 'tensor'), parts along dimension 0
- output 4: float32 [8192, 1024], P(('pod', 'tensor')), parts along dimension 0
There are 2 independent parts. The reference program is written for one: setup_inputs(seed, part) draws one part's arguments, and reference() takes and returns one part's arrays. A program takes and returns all parts, laid end to end along the dimension named above; an argument that names none is the same for every part.
All inputs are finite; a program needn't handle non-finite values.
Results may differ from the reference program's by a relative error of at most 0.00579477.
Values are sent between devices in bfloat16 or wider.
A program may use at most 1 GiB of HBM per device.

```python
import jax
import jax.numpy as jnp
from jax import lax

DATA_WAYS = 4
TENSOR_WAYS = 4
TOK_DEV = 1024
VOCAB_SIZE = 50304
MODEL_DIM = 1024
FFN_DIM = 4096
NORM_EPS = 1e-6
TOKENS_REP = TOK_DEV * TENSOR_WAYS


def gelu_tanh(value):
    return jax.nn.gelu(value, approximate=True)


def draw_ids(id_key):
    k_base, k_shift, k_hot, k_pick, k_use = jax.random.split(id_key, 5)
    total_tok = DATA_WAYS * TOKENS_REP
    base_ids = jax.random.randint(k_base, (total_tok,), 0, VOCAB_SIZE)
    shift_by = jax.random.randint(k_shift, (total_tok,), 0, 3)
    skewed = jnp.right_shift(base_ids, shift_by)
    hot_ids = jax.random.randint(k_hot, (16,), 0, VOCAB_SIZE)
    hot_pick = jax.random.randint(k_pick, (total_tok,), 0, 16)
    use_hot = jax.random.randint(k_use, (total_tok,), 0, 4) == 0
    token_ids = jnp.where(use_hot, hot_ids[hot_pick], skewed)
    token_ids = token_ids.at[0].set(0).at[total_tok - 1].set(VOCAB_SIZE - 1)
    return token_ids.astype(jnp.int32)


def setup_inputs(seed: int = 0, part: int = 0) -> dict:
    root_key = jax.random.key(seed)
    k_table, k_gain, k_in, k_out, k_part = jax.random.split(root_key, 5)
    k_ids, k_grad = jax.random.split(jax.random.fold_in(k_part, part))
    total_tok = DATA_WAYS * TOKENS_REP
    embed_table = jax.random.normal(k_table, (VOCAB_SIZE, MODEL_DIM), jnp.float32).astype(jnp.bfloat16)
    norm_gain = (1.0 + 0.5 * jax.random.uniform(k_gain, (MODEL_DIM,), jnp.float32, -1.0, 1.0)).astype(jnp.bfloat16)
    w_in = (jax.random.normal(k_in, (MODEL_DIM, FFN_DIM), jnp.float32) * MODEL_DIM ** -0.5).astype(jnp.bfloat16)
    w_out = (jax.random.normal(k_out, (FFN_DIM, MODEL_DIM), jnp.float32) * (1.5 * FFN_DIM ** -0.5)).astype(jnp.bfloat16)
    d_out = jax.random.normal(k_grad, (total_tok, MODEL_DIM), jnp.float32).astype(jnp.bfloat16)
    return {"token_ids": draw_ids(k_ids), "embed_table": embed_table, "norm_gain": norm_gain, "w_in": w_in, "w_out": w_out, "d_out": d_out}


def reference(token_ids, embed_table, norm_gain, w_in, w_out, d_out):
    blocks = DATA_WAYS * TENSOR_WAYS
    embedded = jnp.take(embed_table, token_ids, axis=0).reshape(blocks, TOK_DEV, MODEL_DIM)
    grad_blocks = d_out.reshape(blocks, TOK_DEV, MODEL_DIM)
    gain_f32 = norm_gain.astype(jnp.float32)

    def block_step(acc_pair, step_in):
        acc_w_in, acc_w_out = acc_pair
        x_blk, dy_blk = step_in
        x_f32 = x_blk.astype(jnp.float32)
        inv_rms = lax.rsqrt(jnp.mean(x_f32 * x_f32, axis=-1, keepdims=True) + NORM_EPS)
        x_hat = x_f32 * inv_rms
        normed = (x_hat * gain_f32).astype(jnp.bfloat16)
        pre_gelu = jnp.dot(normed, w_in, preferred_element_type=jnp.float32).astype(jnp.bfloat16)
        hidden_f32, gelu_pull = jax.vjp(gelu_tanh, pre_gelu.astype(jnp.float32))
        hidden = hidden_f32.astype(jnp.bfloat16)
        mlp_out = jnp.dot(hidden, w_out, preferred_element_type=jnp.float32)
        out_blk = (x_f32 + mlp_out).astype(jnp.bfloat16)
        grad_hidden = jnp.dot(dy_blk, w_out.T, preferred_element_type=jnp.float32)
        grad_pre = gelu_pull(grad_hidden)[0].astype(jnp.bfloat16)
        acc_w_out = acc_w_out + jnp.dot(hidden.T, dy_blk, preferred_element_type=jnp.float32)
        acc_w_in = acc_w_in + jnp.dot(normed.T, grad_pre, preferred_element_type=jnp.float32)
        d_normed = jnp.dot(grad_pre, w_in.T, preferred_element_type=jnp.float32)
        d_hat = d_normed * gain_f32
        d_norm_in = inv_rms * (d_hat - x_hat * jnp.mean(d_hat * x_hat, axis=-1, keepdims=True))
        dx_blk = (dy_blk.astype(jnp.float32) + d_norm_in).astype(jnp.bfloat16)
        return (acc_w_in, acc_w_out), (out_blk, dx_blk)

    zeros_in = jnp.zeros((MODEL_DIM, FFN_DIM), jnp.float32)
    zeros_out = jnp.zeros((FFN_DIM, MODEL_DIM), jnp.float32)
    (grad_w_in, grad_w_out), (out_blocks, dx_blocks) = lax.scan(block_step, (zeros_in, zeros_out), (embedded, grad_blocks))
    grad_table = jax.ops.segment_sum(dx_blocks.reshape(-1, MODEL_DIM).astype(jnp.float32), token_ids, num_segments=VOCAB_SIZE)
    return out_blocks.reshape(-1, MODEL_DIM), grad_table, grad_w_in, grad_w_out
```

```python
import jax
import jax.numpy as jnp
from jax import lax
from jax.sharding import PartitionSpec as P

NORM_EPS = 1e-6


def gelu_tanh(value):
    return jax.nn.gelu(value, approximate=True)


def solution(mesh):
    tok_spec = P(("pod", "data", "tensor"), None)
    data_ways, tensor_ways = mesh.shape["data"], mesh.shape["tensor"]
    ring = [(i, (i + 1) % data_ways) for i in range(data_ways)]
    tie = lax.optimization_barrier

    def per_device(token_ids, embed_table, norm_gain, w_in, w_out, d_out):
        shard_rows, width = embed_table.shape
        tp_rank = lax.axis_index("tensor")
        dp_rank = lax.axis_index("data")

        def shift(values):
            return [lax.ppermute(value, "data", ring) for value in values]

        def place(index, array):
            rows = array.shape[0] // data_ways
            return lax.rem(index + 2 * data_ways, data_ways) * rows, rows

        def quarter(array, index):
            return lax.dynamic_slice_in_dim(array, *place(index, array), 0)

        grad_all = lax.all_gather(d_out, "tensor", axis=0, tiled=True)
        local_ids = token_ids - tp_rank * shard_rows
        is_owned = (local_ids >= 0) & (local_ids < shard_rows)
        picked = jnp.take(embed_table, jnp.where(is_owned, local_ids, 0), axis=0)
        partial_rows = jnp.where(is_owned[:, None], picked, jnp.zeros_like(picked))
        partial_rows, grad_all, late_ids = tie((partial_rows, grad_all, token_ids))
        embedded = lax.psum_scatter(partial_rows, "tensor", scatter_dimension=0, tiled=True)

        group_ids = lax.all_gather(late_ids, "data", axis=0, tiled=True) - tp_rank * shard_rows
        group_owned = (group_ids >= 0) & (group_ids < shard_rows)
        slots = jnp.where(group_owned, group_ids, shard_rows).reshape(data_ways * tensor_ways, 2, -1)
        slots = [slots[:, half].reshape(-1) for half in range(2)]

        gain_f32 = norm_gain.astype(jnp.float32)
        x_f32 = embedded.astype(jnp.float32)
        inv_rms = lax.rsqrt(jnp.mean(x_f32 * x_f32, axis=-1, keepdims=True) + NORM_EPS)
        x_hat = x_f32 * inv_rms
        normed = (x_hat * gain_f32).astype(jnp.bfloat16)
        normed_all = lax.all_gather(normed, "tensor", axis=0, tiled=True)
        pre_gelu = jnp.dot(normed_all, w_in, preferred_element_type=jnp.float32).astype(jnp.bfloat16)
        hidden_f32, gelu_pull = jax.vjp(gelu_tanh, pre_gelu.astype(jnp.float32))
        hidden = hidden_f32.astype(jnp.bfloat16)
        grad_hidden = lax.dot_general(grad_all, w_out, (((1,), (1,)), ((), ())), preferred_element_type=jnp.float32)
        grad_pre = gelu_pull(grad_hidden)[0].astype(jnp.bfloat16)
        norm_part = lax.dot_general(grad_pre, w_in, (((1,), (1,)), ((), ())), preferred_element_type=jnp.float32)
        d_normed = lax.psum_scatter(norm_part, "tensor", scatter_dimension=0, tiled=True)

        grads = [
            lax.dot_general(hidden, grad_all, (((0,), (0,)), ((), ())), preferred_element_type=jnp.float32),
            lax.dot_general(normed_all, grad_pre, (((0,), (0,)), ((), ())), preferred_element_type=jnp.float32),
        ]
        moving = [quarter(grad, dp_rank) for grad in grads]
        for step in (1, 2):
            moving = [got + quarter(grad, dp_rank - step) for got, grad in zip(shift(moving), grads)]
        mlp_part = jnp.dot(hidden, w_out, preferred_element_type=jnp.float32)
        d_normed, mlp_part, moving, slots = tie((d_normed, mlp_part, moving, slots))

        moving = [got + quarter(grad, dp_rank - 3) for got, grad in zip(shift(moving), grads)]
        d_hat = d_normed * gain_f32
        d_norm_in = inv_rms * (d_hat - x_hat * jnp.mean(d_hat * x_hat, axis=-1, keepdims=True))
        d_embed = (d_out.astype(jnp.float32) + d_norm_in).astype(jnp.bfloat16)
        pieces = d_embed.reshape(2, -1, width)
        rows = lax.all_gather(pieces[0], ("data", "tensor"), axis=0, tiled=True)
        rows, piece, moving = tie((rows, pieces[1], moving))

        done = [moving]
        moving = shift(moving)
        next_rows = lax.all_gather(piece, ("data", "tensor"), axis=0, tiled=True)
        grad_table = jnp.zeros((shard_rows, width), jnp.float32)
        grad_table = grad_table.at[slots[0]].add(rows.astype(jnp.float32), mode="drop")
        grad_table, next_rows, moving, mlp_part = tie((grad_table, next_rows, moving, mlp_part))

        mlp_out = lax.psum_scatter(mlp_part, "tensor", scatter_dimension=0, tiled=True)
        done.append(moving)
        for _ in (5, 6):
            moving = shift(moving)
            done.append(moving)
        grad_table = grad_table.at[slots[1]].add(next_rows.astype(jnp.float32), mode="drop")
        block_out = (x_f32 + mlp_out).astype(jnp.bfloat16)
        sums = []
        for which, grad in enumerate(grads):
            total = jnp.zeros_like(grad)
            for step, parts in enumerate(done):
                total = lax.dynamic_update_slice_in_dim(total, parts[which], place(dp_rank + 1 - step, grad)[0], 0)
            sums.append(total)
        return block_out, grad_table, sums[1], sums[0]

    return jax.shard_map(
        per_device,
        mesh=mesh,
        in_specs=(P(("pod", "data")), P("tensor", None), P(None), P(None, "tensor"), P("tensor", None), tok_spec),
        out_specs=(tok_spec, P(("pod", "tensor"), None), P("pod", "tensor"), P(("pod", "tensor"), None)),
        check_vma=False,
    )
```

```python
import jax
import jax.numpy as jnp
from jax import lax
from jax.sharding import PartitionSpec as P

NORM_EPS = 1e-6
ROW_SHARES = (11, 10, 7, 4)
SUM_PIECES = 2


def gelu_tanh(value):
    return jax.nn.gelu(value, approximate=True)


def solution(mesh):
    tok_spec = P(("pod", "data", "tensor"), None)
    data_ways, tensor_ways = mesh.shape["data"], mesh.shape["tensor"]
    tie = lax.optimization_barrier

    def per_device(token_ids, embed_table, norm_gain, w_in, w_out, d_out):
        shard_rows, width = embed_table.shape
        tp_rank = lax.axis_index("tensor")
        dp_rank = lax.axis_index("data")

        def send_in(part):
            return part + lax.ppermute(part, "data", [(0, 1), (3, 2)])

        def swap(half):
            return half + lax.ppermute(half, "data", [(1, 2), (2, 1)])

        def send_out(total):
            inner = (dp_rank == 1) | (dp_rank == 2)
            return jnp.where(inner, total, lax.ppermute(total, "data", [(1, 0), (2, 3)]))

        grad_all = lax.all_gather(d_out, "tensor", axis=0, tiled=True)
        local_ids = token_ids - tp_rank * shard_rows
        is_owned = (local_ids >= 0) & (local_ids < shard_rows)
        picked = jnp.take(embed_table, jnp.where(is_owned, local_ids, 0), axis=0)
        partial_rows = jnp.where(is_owned[:, None], picked, jnp.zeros_like(picked))
        partial_rows, grad_all, late_ids = tie((partial_rows, grad_all, token_ids))
        embedded = lax.psum_scatter(partial_rows, "tensor", scatter_dimension=0, tiled=True)

        group_ids = lax.all_gather(late_ids, "data", axis=0, tiled=True) - tp_rank * shard_rows
        group_owned = (group_ids >= 0) & (group_ids < shard_rows)
        slots = jnp.where(group_owned, group_ids, shard_rows).reshape(data_ways * tensor_ways, -1)

        embedded, slots = tie((embedded, slots))
        gain_f32 = norm_gain.astype(jnp.float32)
        x_f32 = embedded.astype(jnp.float32)
        inv_rms = lax.rsqrt(jnp.mean(x_f32 * x_f32, axis=-1, keepdims=True) + NORM_EPS)
        x_hat = x_f32 * inv_rms
        normed = (x_hat * gain_f32).astype(jnp.bfloat16)
        normed_all = lax.all_gather(normed, "tensor", axis=0, tiled=True)
        pre_gelu = jnp.dot(normed_all, w_in, preferred_element_type=jnp.float32).astype(jnp.bfloat16)
        hidden_f32, gelu_pull = jax.vjp(gelu_tanh, pre_gelu.astype(jnp.float32))
        hidden = hidden_f32.astype(jnp.bfloat16)
        grad_hidden = lax.dot_general(grad_all, w_out, (((1,), (1,)), ((), ())), preferred_element_type=jnp.float32)
        grad_pre = gelu_pull(grad_hidden)[0].astype(jnp.bfloat16)
        norm_part = lax.dot_general(grad_pre, w_in, (((1,), (1,)), ((), ())), preferred_element_type=jnp.float32)
        norm_part, hidden = tie((norm_part, hidden))
        d_normed = lax.psum_scatter(norm_part, "tensor", scatter_dimension=0, tiled=True)

        parts = []
        for left, right in ((hidden, grad_all), (normed_all, grad_pre)):
            grad = lax.dot_general(left, right, (((0,), (0,)), ((), ())), preferred_element_type=jnp.float32)
            rows = grad.shape[0] // SUM_PIECES
            cut, hidden = tie(([grad[at * rows : (at + 1) * rows] for at in range(SUM_PIECES)], hidden))
            parts += cut
        first, hidden = tie((send_in(parts[0]), hidden))
        mlp_part = jnp.dot(hidden, w_out, preferred_element_type=jnp.float32)
        mlp_out = lax.psum_scatter(mlp_part, "tensor", scatter_dimension=0, tiled=True)

        halves = [first] + [send_in(part) for part in parts[1:3]]
        totals = [swap(half) for half in halves[:2]]
        sent = [send_out(totals[0])]
        d_normed, halves, totals, sent = tie((d_normed, halves, totals, sent))

        d_hat = d_normed * gain_f32
        d_norm_in = inv_rms * (d_hat - x_hat * jnp.mean(d_hat * x_hat, axis=-1, keepdims=True))
        d_embed = (d_out.astype(jnp.float32) + d_norm_in).astype(jnp.bfloat16)
        halves.append(send_in(parts[3]))
        totals += [swap(half) for half in halves[2:]]
        sent += [send_out(total) for total in totals[1:3]]
        d_embed, mlp_out, totals, sent = tie((d_embed, mlp_out, totals, sent))
        sent.append(send_out(totals[3]))
        sums = [jnp.concatenate([sent[at + index] for index in range(SUM_PIECES)]) for at in (0, SUM_PIECES)]
        block_out = (x_f32 + mlp_out).astype(jnp.bfloat16)

        pieces, places, start = [], [], 0
        for share in ROW_SHARES:
            size = d_embed.shape[0] * share // sum(ROW_SHARES)
            pieces.append(d_embed[start : start + size])
            places.append(slots[:, start : start + size].reshape(-1))
            start += size
        grad_table = jnp.zeros((shard_rows, width), jnp.float32)
        piece = pieces[0]
        for step, place in enumerate(places):
            rows = lax.all_gather(piece, ("data", "tensor"), axis=0, tiled=True)
            if step:
                rows, grad_table = tie((rows, grad_table))
            else:
                rows, sums = tie((rows, sums))
            if step + 1 < len(places):
                rows, piece = tie((rows, pieces[step + 1]))
            grad_table = grad_table.at[place].add(rows.astype(jnp.float32), mode="drop")
        return block_out, grad_table, sums[1], sums[0]

    return jax.shard_map(
        per_device,
        mesh=mesh,
        in_specs=(P(("pod", "data")), P("tensor", None), P(None), P(None, "tensor"), P("tensor", None), tok_spec),
        out_specs=(tok_spec, P(("pod", "tensor"), None), P("pod", "tensor"), P(("pod", "tensor"), None)),
        check_vma=False,
    )
```

```python
import jax
import jax.numpy as jnp
from jax import lax
from jax.sharding import PartitionSpec as P

NORM_EPS = 1e-6
CHUNKS = 4


def gelu_tanh(value):
    return jax.nn.gelu(value, approximate=True)


def solution(mesh):
    tok_spec = P(("pod", "data", "tensor"), None)
    data_ways, tensor_ways = mesh.shape["data"], mesh.shape["tensor"]
    ring = [(i, (i + 1) % data_ways) for i in range(data_ways)]
    tie = lax.optimization_barrier

    def per_device(token_ids, embed_table, norm_gain, w_in, w_out, d_out):
        shard_rows, width = embed_table.shape
        tp_rank = lax.axis_index("tensor")
        dp_rank = lax.axis_index("data")

        def shift(values):
            return [lax.ppermute(value, "data", ring) for value in values]

        def place(index, array):
            rows = array.shape[0] // data_ways
            return lax.rem(index + 2 * data_ways, data_ways) * rows, rows

        def quarter(array, index):
            return lax.dynamic_slice_in_dim(array, *place(index, array), 0)

        grad_all = lax.all_gather(d_out, "tensor", axis=0, tiled=True)
        local_ids = token_ids - tp_rank * shard_rows
        is_owned = (local_ids >= 0) & (local_ids < shard_rows)
        picked = jnp.take(embed_table, jnp.where(is_owned, local_ids, 0), axis=0)
        partial_rows = jnp.where(is_owned[:, None], picked, jnp.zeros_like(picked))
        partial_rows, grad_all, late_ids = tie((partial_rows, grad_all, token_ids))
        embedded = lax.psum_scatter(partial_rows, "tensor", scatter_dimension=0, tiled=True)

        group_ids = lax.all_gather(late_ids, "data", axis=0, tiled=True) - tp_rank * shard_rows
        group_owned = (group_ids >= 0) & (group_ids < shard_rows)
        slots = jnp.where(group_owned, group_ids, shard_rows).reshape(data_ways * tensor_ways, -1)
        embedded, slots = tie((embedded, slots))

        gain_f32 = norm_gain.astype(jnp.float32)
        x_f32 = embedded.astype(jnp.float32)
        inv_rms = lax.rsqrt(jnp.mean(x_f32 * x_f32, axis=-1, keepdims=True) + NORM_EPS)
        x_hat = x_f32 * inv_rms
        normed = (x_hat * gain_f32).astype(jnp.bfloat16)
        normed_all = lax.all_gather(normed, "tensor", axis=0, tiled=True)
        pre_gelu = jnp.dot(normed_all, w_in, preferred_element_type=jnp.float32).astype(jnp.bfloat16)
        hidden_f32, gelu_pull = jax.vjp(gelu_tanh, pre_gelu.astype(jnp.float32))
        hidden = hidden_f32.astype(jnp.bfloat16)
        grad_hidden = lax.dot_general(grad_all, w_out, (((1,), (1,)), ((), ())), preferred_element_type=jnp.float32)
        grad_pre = gelu_pull(grad_hidden)[0].astype(jnp.bfloat16)
        norm_part = lax.dot_general(grad_pre, w_in, (((1,), (1,)), ((), ())), preferred_element_type=jnp.float32)
        d_normed = lax.psum_scatter(norm_part, "tensor", scatter_dimension=0, tiled=True)

        grads = [
            lax.dot_general(hidden, grad_all, (((0,), (0,)), ((), ())), preferred_element_type=jnp.float32),
            lax.dot_general(normed_all, grad_pre, (((0,), (0,)), ((), ())), preferred_element_type=jnp.float32),
        ]
        moving = [quarter(grad, dp_rank) for grad in grads]
        for step in (1, 2):
            moving = [got + quarter(grad, dp_rank - step) for got, grad in zip(shift(moving), grads)]
        mlp_part = jnp.dot(hidden, w_out, preferred_element_type=jnp.float32)
        half_rows = d_out.shape[0] // 2
        mlp_halves = mlp_part.reshape(tensor_ways, 2, half_rows, width)
        mlp_halves = [mlp_halves[:, half].reshape(-1, width) for half in range(2)]
        d_normed, mlp_halves, moving = tie((d_normed, mlp_halves, moving))

        mlp_low = lax.psum_scatter(mlp_halves[0], "tensor", scatter_dimension=0, tiled=True)
        moving = [got + quarter(grad, dp_rank - 3) for got, grad in zip(shift(moving), grads)]
        d_hat = d_normed * gain_f32
        d_norm_in = inv_rms * (d_hat - x_hat * jnp.mean(d_hat * x_hat, axis=-1, keepdims=True))
        d_embed = (d_out.astype(jnp.float32) + d_norm_in).astype(jnp.bfloat16)

        def over_data(piece):
            return [lax.ppermute(piece, "data", [(i, (i - by) % data_ways) for i in range(data_ways)]) for by in (1, 2, 3)]

        def gather_block(piece, jumps):
            rows = piece.shape[0]
            out = jnp.zeros((data_ways * rows, width), piece.dtype)
            for by, part in enumerate([piece] + jumps):
                out = lax.dynamic_update_slice_in_dim(out, part, lax.rem(dp_rank + by, data_ways) * rows, 0)
            return out

        size = d_embed.shape[0] // CHUNKS
        pieces = [d_embed[chunk * size : (chunk + 1) * size] for chunk in range(CHUNKS)]
        jumps = [over_data(piece) for piece in pieces]
        slots = slots.reshape(data_ways, tensor_ways, CHUNKS, size).transpose(2, 1, 0, 3).reshape(CHUNKS, -1)
        block, mlp_low, pieces, moving = tie((gather_block(pieces[0], jumps[0]), mlp_low, pieces, moving))
        later = gather_block(pieces[1], jumps[1])
        grad_table = jnp.zeros((shard_rows, width), jnp.float32)
        done = []
        for chunk in range(CHUNKS):
            rows = lax.all_gather(block, "tensor", axis=0, tiled=True)
            if chunk == 0:
                rows, block = tie((rows, later))
            elif chunk < CHUNKS - 1:
                rows, grad_table, block, moving = tie((rows, grad_table, later, moving))
            else:
                rows, grad_table, mlp_high, moving = tie((rows, grad_table, mlp_halves[1], moving))
                mlp_high = lax.psum_scatter(mlp_high, "tensor", scatter_dimension=0, tiled=True)
            if chunk:
                done.append(moving)
                moving = shift(moving)
            grad_table = grad_table.at[slots[chunk]].add(rows.astype(jnp.float32), mode="drop")
            if chunk + 2 < CHUNKS:
                grad_table, piece = tie((grad_table, pieces[chunk + 2]))
                later = gather_block(piece, jumps[chunk + 2])
        done.append(moving)
        block_out = (x_f32 + jnp.concatenate([mlp_low, mlp_high])).astype(jnp.bfloat16)
        sums = []
        for which, grad in enumerate(grads):
            total = jnp.zeros_like(grad)
            for step, parts in enumerate(done):
                total = lax.dynamic_update_slice_in_dim(total, parts[which], place(dp_rank + 1 - step, grad)[0], 0)
            sums.append(total)
        return block_out, grad_table, sums[1], sums[0]

    return jax.shard_map(
        per_device,
        mesh=mesh,
        in_specs=(P(("pod", "data")), P("tensor", None), P(None), P(None, "tensor"), P("tensor", None), tok_spec),
        out_specs=(tok_spec, P(("pod", "tensor"), None), P("pod", "tensor"), P(("pod", "tensor"), None)),
        check_vma=False,
    )
```

```python
import jax
import jax.numpy as jnp
from jax import lax
from jax.sharding import PartitionSpec as P

NORM_EPS = 1e-6
SHARES = (21, 21, 22)


def gelu_tanh(value):
    return jax.nn.gelu(value, approximate=True)


def solution(mesh):
    tok_spec = P(("pod", "data", "tensor"), None)
    data_ways, tensor_ways = mesh.shape["data"], mesh.shape["tensor"]
    ring = [(i, (i + 1) % data_ways) for i in range(data_ways)]
    tie = lax.optimization_barrier

    def per_device(token_ids, embed_table, norm_gain, w_in, w_out, d_out):
        shard_rows, width = embed_table.shape
        tp_rank = lax.axis_index("tensor")
        dp_rank = lax.axis_index("data")

        def shift(values):
            return [lax.ppermute(value, "data", ring) for value in values]

        def place(index, array):
            rows = array.shape[0] // data_ways
            return lax.rem(index + 2 * data_ways, data_ways) * rows, rows

        def quarter(array, index):
            return lax.dynamic_slice_in_dim(array, *place(index, array), 0)

        grad_all = lax.all_gather(d_out, "tensor", axis=0, tiled=True)
        local_ids = token_ids - tp_rank * shard_rows
        is_owned = (local_ids >= 0) & (local_ids < shard_rows)
        picked = jnp.take(embed_table, jnp.where(is_owned, local_ids, 0), axis=0)
        partial_rows = jnp.where(is_owned[:, None], picked, jnp.zeros_like(picked))
        partial_rows, grad_all, late_ids = tie((partial_rows, grad_all, token_ids))
        embedded = lax.psum_scatter(partial_rows, "tensor", scatter_dimension=0, tiled=True)

        group_ids = lax.all_gather(late_ids, "data", axis=0, tiled=True) - tp_rank * shard_rows
        group_owned = (group_ids >= 0) & (group_ids < shard_rows)
        slots = jnp.where(group_owned, group_ids, shard_rows).reshape(data_ways * tensor_ways, -1)
        embedded, slots = tie((embedded, slots))

        gain_f32 = norm_gain.astype(jnp.float32)
        x_f32 = embedded.astype(jnp.float32)
        inv_rms = lax.rsqrt(jnp.mean(x_f32 * x_f32, axis=-1, keepdims=True) + NORM_EPS)
        x_hat = x_f32 * inv_rms
        normed = (x_hat * gain_f32).astype(jnp.bfloat16)
        normed_all = lax.all_gather(normed, "tensor", axis=0, tiled=True)
        pre_gelu = jnp.dot(normed_all, w_in, preferred_element_type=jnp.float32).astype(jnp.bfloat16)
        hidden_f32, gelu_pull = jax.vjp(gelu_tanh, pre_gelu.astype(jnp.float32))
        hidden = hidden_f32.astype(jnp.bfloat16)
        grad_hidden = lax.dot_general(grad_all, w_out, (((1,), (1,)), ((), ())), preferred_element_type=jnp.float32)
        grad_pre = gelu_pull(grad_hidden)[0].astype(jnp.bfloat16)
        norm_part = lax.dot_general(grad_pre, w_in, (((1,), (1,)), ((), ())), preferred_element_type=jnp.float32)
        d_normed = lax.psum_scatter(norm_part, "tensor", scatter_dimension=0, tiled=True)

        grads = [
            lax.dot_general(hidden, grad_all, (((0,), (0,)), ((), ())), preferred_element_type=jnp.float32),
            lax.dot_general(normed_all, grad_pre, (((0,), (0,)), ((), ())), preferred_element_type=jnp.float32),
        ]
        moving = [quarter(grad, dp_rank) for grad in grads]
        for step in (1, 2):
            moving = [got + quarter(grad, dp_rank - step) for got, grad in zip(shift(moving), grads)]
        mlp_part = jnp.dot(hidden, w_out, preferred_element_type=jnp.float32)
        half_rows = d_out.shape[0] // 2
        mlp_halves = mlp_part.reshape(tensor_ways, 2, half_rows, width)
        mlp_halves = [mlp_halves[:, half].reshape(-1, width) for half in range(2)]
        d_normed, mlp_halves, moving = tie((d_normed, mlp_halves, moving))

        mlp_low = lax.psum_scatter(mlp_halves[0], "tensor", scatter_dimension=0, tiled=True)
        moving = [got + quarter(grad, dp_rank - 3) for got, grad in zip(shift(moving), grads)]
        d_hat = d_normed * gain_f32
        d_norm_in = inv_rms * (d_hat - x_hat * jnp.mean(d_hat * x_hat, axis=-1, keepdims=True))
        d_embed = (d_out.astype(jnp.float32) + d_norm_in).astype(jnp.bfloat16)

        def over_data(piece):
            return [lax.ppermute(piece, "data", [(i, (i - by) % data_ways) for i in range(data_ways)]) for by in (1, 2, 3)]

        def gather_block(piece, jumps):
            rows = piece.shape[0]
            out = jnp.zeros((data_ways * rows, width), piece.dtype)
            for by, part in enumerate([piece] + jumps):
                out = lax.dynamic_update_slice_in_dim(out, part, lax.rem(dp_rank + by, data_ways) * rows, 0)
            return out

        slots = slots.reshape(data_ways, tensor_ways, -1)
        pieces, places, start = [], [], 0
        for share in SHARES:
            stop = start + d_embed.shape[0] * share // sum(SHARES)
            pieces.append(d_embed[start:stop])
            places.append(slots[:, :, start:stop].transpose(1, 0, 2).reshape(-1))
            start = stop
        jumps = [over_data(piece) for piece in pieces]
        block, mlp_low, pieces, moving = tie((gather_block(pieces[0], jumps[0]), mlp_low, pieces, moving))
        later = gather_block(pieces[1], jumps[1])
        grad_table = jnp.zeros((shard_rows, width), jnp.float32)
        sums = [jnp.zeros_like(grad) for grad in grads]

        def put(step):
            return [
                lax.dynamic_update_slice_in_dim(total, part, place(dp_rank + 1 - step, total)[0], 0)
                for total, part in zip(sums, moving)
            ]

        sums = put(0)
        for chunk, spots in enumerate(places):
            rows = lax.all_gather(block, "tensor", axis=0, tiled=True)
            if chunk == 0:
                rows, block, moving, sums = tie((rows, later, moving, sums))
            elif chunk + 1 < len(places):
                rows, grad_table, block, moving = tie((rows, grad_table, later, moving))
            else:
                rows, grad_table, mlp_high, moving = tie((rows, grad_table, mlp_halves[1], moving))
                mlp_high = lax.psum_scatter(mlp_high, "tensor", scatter_dimension=0, tiled=True)
            if chunk:
                sums = put(chunk)
            moving = shift(moving)
            grad_table = grad_table.at[spots].add(rows.astype(jnp.float32), mode="drop")
            if chunk + 2 < len(places):
                grad_table, piece = tie((grad_table, pieces[chunk + 2]))
                later = gather_block(piece, jumps[chunk + 2])
        sums = put(len(places))
        block_out = (x_f32 + jnp.concatenate([mlp_low, mlp_high])).astype(jnp.bfloat16)
        return block_out, grad_table, sums[1], sums[0]

    return jax.shard_map(
        per_device,
        mesh=mesh,
        in_specs=(P(("pod", "data")), P("tensor", None), P(None), P(None, "tensor"), P("tensor", None), tok_spec),
        out_specs=(tok_spec, P(("pod", "tensor"), None), P("pod", "tensor"), P(("pod", "tensor"), None)),
        check_vma=False,
    )
```
